32 devices in a mesh: fem: 4 (over y, x), bem: 8 (over z, core).
Axes of the slice: x: 2, y: 2, z: 4, core: 2. Of those that a mesh axis runs over, the one named last changes fastest.
Arguments:
- fem_field: float32 [32, 64, 32, 128], P('fem', 'bem'), may hold values from -6 to 6
- fem_source: float32 [32, 64, 32, 128], P('fem', 'bem'), may hold values from -6 to 6
- reaction: float32 [32, 64, 32], P('fem', 'bem'), may hold values from 0.5 to 3
- bem_density: float32 [128, 8192], P(None, 'bem'), may hold values from -6 to 6
- bem_source: float32 [128, 8192], P(None, 'bem'), may hold values from -6 to 6
- bem_diagonal: float32 [8192], P('bem'), may hold values from 2 to 6
- near_blocks: bfloat16 [16, 48, 512, 512], P('bem', 'fem'), may hold values from -0.0390625 to 0.0390625
- near_pairs: int32 [16, 48], P('bem'), may hold values from 0 to 15, as said below
- low_left: bfloat16 [16, 32, 512], P('bem'), may hold values from -1 to 1
- low_right: bfloat16 [16, 32, 512], replicated, may hold values from -0.25 to 0.25
- centers: float32 [16, 3], replicated, may hold values from 0 to 4
- trace_cell: int32 [8192], P(('fem', 'bem')), may hold values from 0 to 2047
- trace_bank: int32 [8192, 1], P(('fem', 'bem')), may hold values from 0 to 7; in each aligned block of 256 rows (0 to 255, 256 to 511, ...) at most 32 rows name the same one
- trace_row: int32 [8192], P(('fem', 'bem')), may hold values from 0 to 1023
Outputs:
- fem_out: float32 [32, 64, 32, 128], P('fem', 'bem')
- bem_out: float32 [128, 8192], P('fem', 'bem')
The draws below stay inside these ranges and needn't reach their ends.
Inputs may be any that keep to these rules, and one draw needn't show every extreme that they name: `trace_bank`: among the 256 slots of one device no bem index is named more than 32 times, and some device names some index exactly 32 times. Panel p's near-field source panels are held by bem indices within two of p's own, counted around the bem axis: near_pairs[p, k] // 2 - p // 2 is -2, -1, 0, 1 or 2 modulo 8.
All inputs are finite; a program needn't handle non-finite values.
Results may differ from the reference program's by a relative error of at most 0.0028.
Values may be sent and summed in bfloat16 or wider, within the bound.
A program may use at most 128 MiB of HBM per device.

```python
import math
import jax
import jax.numpy as jnp
import numpy as np
from jax import lax

E = 128
CX = 8
CY = 8
CZ = 32
PANEL = 512
RANK = 32
NEAR = 48
PANEL_DEV = 2
TR_DEV = 256
CAP = 32
ITERS = 3
NX = 32
NY = 64
PANELS = 16
NB = 8192
SLOTS = 8192
N_FEM = 4
N_BEM = 8


def draw_near_pairs(key, part):
    home = jnp.arange(PANELS, dtype=jnp.int32)[:, None] // PANEL_DEV
    offset_bank = jax.random.randint(jax.random.fold_in(key, 11), (PANELS, NEAR), -2, 3)
    within = jax.random.randint(jax.random.fold_in(key, 12), (PANELS, NEAR), 0, PANEL_DEV)
    return ((home + offset_bank) % N_BEM * PANEL_DEV + within).astype(jnp.int32)


def with_ends(values, own_key, low, top_value):
    shape = values.shape
    place = [jax.random.randint(jax.random.fold_in(own_key, axis), (), 0, shape[axis]) for axis in range(len(shape))]
    values = values.at[tuple(place)].set(low)
    longest = shape.index(max(shape))
    place[longest] = (place[longest] + 1) % shape[longest]
    return values.at[tuple(place)].set(top_value)


def block_levels(rng, extent, cuts, least, high):
    def one(position, blocks):
        heights = jax.random.uniform(jax.random.fold_in(jax.random.fold_in(rng, 6), position), (blocks,), jnp.float32, least / len(cuts), high / len(cuts))
        return jnp.repeat(jnp.exp(heights), extent[position] // blocks).reshape((-1,) + (1,) * (len(extent) - position - 1))

    level = one(*cuts[0])
    for cut in cuts[1:]:
        level = level * one(*cut)
    return level


def shared_out(rng, own, number, rows, count, top, reach, skew):
    ranking = jax.random.permutation(rng, count)
    packed, ordinary = load_shares(count, rows * top, reach, skew, True), load_shares(count, rows * top, reach, skew, False)
    places = jnp.arange(count)

    def named(sizes, offset_by):
        used = int((sizes > 0).sum())
        fixed = max(1, used // 4)
        passed = fixed + (places - fixed + offset_by * (used - fixed)) % max(1, count - fixed)
        return jnp.zeros((count,), jnp.int32).at[ranking[jnp.where(places < fixed, places, passed)]].set(jnp.asarray(sizes, jnp.int32))

    sizes = jnp.where(number % 4 == 0, named(packed, number // 4), named(ordinary, number - number // 4 - 1))
    mixed = jax.random.permutation(jax.random.fold_in(own, 3), count)
    giver, sink = mixed[0:count // 2 * 2:2], mixed[1:count // 2 * 2:2]
    margin = jnp.minimum(sizes[giver] - 1, reach - sizes[sink]) // 2
    margin = jnp.where((giver == ranking[0]) | (sink == ranking[0]) | (sizes[sink] == 0), 0, jnp.maximum(margin, 0))
    passed = jax.random.randint(jax.random.fold_in(own, 4), (count // 2,), 0, 1 << 20) % (margin + 1)
    sizes = sizes.at[giver].add(-passed).at[sink].add(passed)
    labels = jnp.searchsorted(jnp.cumsum(sizes), jnp.arange(rows * top), side="right").astype(jnp.int32)
    table = labels.reshape(top, rows).T
    table = table[jax.random.permutation(jax.random.fold_in(own, 1), rows)]
    offset_by = jax.random.randint(jax.random.fold_in(own, 2), (rows, 1), 0, top)
    return jnp.take_along_axis(table, (jnp.arange(top)[None, :] + offset_by) % top, axis=1)


def load_shares(count, total, most, lean, full):
    weights = [(1 << 20) // math.isqrt(standing ** lean) + 1 for standing in range(1, count + 1)]
    largest = most if full else min(most, max(-(-total // count), total * weights[0] // sum(weights)))
    least = 1 if total - largest >= count - 1 else 0
    counts, rest = [largest] + [least] * (count - 1), total - largest - least * (count - 1)
    while rest > 0:
        candidates = [i for i in range(1, count) if counts[i] < largest] or [i for i in range(1, count) if counts[i] < most]
        mass, budget = sum([weights[i] for i in candidates]), rest
        for i in candidates:
            extra = min(most - counts[i], max(1, budget * weights[i] // mass), rest)
            counts[i] = counts[i] + extra
            rest = rest - extra
    return np.array(counts)


def gaussian(own_key, shape, spread, most, shards=(), kind=jnp.bfloat16):
    drawn = spread * jax.random.normal(own_key, shape, jnp.float32)
    if shards:
        drawn = drawn * block_levels(own_key, shape, shards, -0.22, 0.18)
    return jnp.clip(drawn, -most, most).astype(kind)


def setup_inputs(seed: int = 0) -> dict:
    seeds = jax.random.split(jax.random.key(seed), 15)
    fem_field = gaussian(seeds[0], (NX, NY, CZ, E), 1.0, 6.0, ((0, 4), (1, 8)), jnp.float32)
    fem_source = gaussian(seeds[1], (NX, NY, CZ, E), 1.0, 6.0, ((0, 4), (1, 8)), jnp.float32)
    reaction = jnp.clip(0.5 + 2.5 * jax.random.uniform(seeds[2], (NX, NY, CZ), jnp.float32) ** block_levels(seeds[2], (NX, NY, CZ), ((0, 4), (1, 8)), -0.2, 0.2), 0.5, 3.0)
    bem_density = gaussian(seeds[3], (E, NB), 1.0, 6.0, ((1, 8),), jnp.float32)
    bem_source = gaussian(seeds[4], (E, NB), 1.0, 6.0, ((1, 8),), jnp.float32)
    bem_diagonal = jnp.clip(jnp.exp(math.log(6.0) - 1.0986123 * jax.random.uniform(seeds[5], (NB,), jnp.float32) ** block_levels(seeds[5], (NB,), ((0, 8),), -0.2, 0.2)), 2.0, 6.0)
    near_blocks = gaussian(seeds[6], (PANELS, NEAR, PANEL, PANEL), (NEAR * PANEL) ** -0.5, 0.0390625, ((0, 8), (1, 4)))
    near_pairs = draw_near_pairs(jax.random.fold_in(seeds[14], 71), 0)
    low_left = gaussian(seeds[8], (PANELS, RANK, PANEL), RANK ** -0.5, 1.0, ((0, 8),))
    low_right = gaussian(seeds[9], (PANELS, RANK, PANEL), PANEL ** -0.5, 0.25)
    centers = jnp.clip(jax.random.uniform(seeds[10], (PANELS, 3), jnp.float32, 0.0, 4.0), 0.0, 4.0)
    trace_cell = with_ends(jax.random.randint(seeds[11], (SLOTS,), 0, CX * CY * CZ), jax.random.fold_in(seeds[11], 1), 0, (CX * CY * CZ) - 1).astype(jnp.int32)
    trace_bank_keys = jax.random.split(jax.random.fold_in(seeds[12], 1), SLOTS // TR_DEV)
    trace_bank_turns = jax.random.permutation(jax.random.fold_in(seeds[12], 3), SLOTS // TR_DEV)
    trace_bank = jax.vmap(lambda own, number: shared_out(jax.random.fold_in(seeds[12], 2), own, number, TR_DEV, N_BEM, 1, CAP, 2))(trace_bank_keys, trace_bank_turns).reshape((SLOTS, 1))
    trace_row = with_ends(jax.random.randint(seeds[13], (SLOTS,), 0, PANEL_DEV * PANEL), jax.random.fold_in(seeds[13], 1), 0, (PANEL_DEV * PANEL) - 1).astype(jnp.int32)
    return dict(fem_field=fem_field, fem_source=fem_source, reaction=reaction, bem_density=bem_density, bem_source=bem_source, bem_diagonal=bem_diagonal, near_blocks=near_blocks, near_pairs=near_pairs, low_left=low_left, low_right=low_right, centers=centers, trace_cell=trace_cell, trace_bank=trace_bank, trace_row=trace_row)


HIGHEST = lax.Precision.HIGHEST


def stiffness(state, reaction):
    padded = jnp.pad(state, ((1, 1), (1, 1), (1, 1), (0, 0)))
    beside = padded[2:, 1:-1, 1:-1] + padded[:-2, 1:-1, 1:-1]
    beside = beside + padded[1:-1, 2:, 1:-1] + padded[1:-1, :-2, 1:-1]
    beside = beside + padded[1:-1, 1:-1, 2:] + padded[1:-1, 1:-1, :-2]
    return (6.0 + reaction)[..., None] * state - beside


def by_device(state):
    blocks = state.reshape(N_FEM, CX, N_BEM, CY, CZ, E).transpose(0, 2, 1, 3, 4, 5)
    return blocks.reshape(N_FEM * N_BEM * CX * CY * CZ, E)


def from_device(flat):
    blocks = flat.reshape(N_FEM, N_BEM, CX, CY, CZ, E).transpose(0, 2, 1, 3, 4, 5)
    return blocks.reshape(N_FEM * CX, N_BEM * CY, CZ, E)


def near_field(rounded, near_blocks, near_pairs):
    grouped = rounded.reshape(E, PANELS, PANEL)

    def one_panel(pieces):
        blocks, pairs = pieces
        chosen = jnp.take(grouped, pairs, axis=1).astype(jnp.float32)
        return jnp.einsum("ekn,knm->em", chosen, blocks.astype(jnp.float32), precision=HIGHEST)

    rows = lax.map(one_panel, (near_blocks, near_pairs))
    return rows.transpose(1, 0, 2).reshape(E, PANELS * PANEL)


def far_field(rounded, low_left, low_right, centers, near_pairs):
    grouped = rounded.reshape(E, PANELS, PANEL).astype(jnp.float32)
    reduced = jnp.einsum("eqn,qrn->eqr", grouped, low_right.astype(jnp.float32), precision=HIGHEST).astype(jnp.bfloat16)
    reduced = lax.optimization_barrier(reduced).astype(jnp.float32)
    offsets = centers[:, None, :] - centers[None, :, :]
    kernel = 1.0 / (1.0 + jnp.sum(offsets * offsets, axis=-1))
    panel_ids = jnp.arange(PANELS, dtype=jnp.int32)
    listed = jnp.any(near_pairs[:, :, None] == panel_ids[None, None, :], axis=1)
    listed = listed | (panel_ids[:, None] == panel_ids[None, :])
    kernel = jnp.where(listed, 0.0, kernel)
    weights = jnp.einsum("pq,eqr->epr", kernel, reduced, precision=HIGHEST)
    distant = jnp.einsum("epr,prn->epn", weights, low_left.astype(jnp.float32), precision=HIGHEST)
    return distant.reshape(E, PANELS * PANEL)


def reference(fem_field, fem_source, reaction, bem_density, bem_source, bem_diagonal, near_blocks, near_pairs, low_left, low_right, centers, trace_cell, trace_bank, trace_row):
    slot_device = jnp.arange(trace_cell.shape[0], dtype=jnp.int32) // TR_DEV
    cell_index = (slot_device * (CX * CY * CZ) + trace_cell).astype(jnp.int32)
    node_index = (trace_bank[:, 0] * (PANEL_DEV * PANEL) + trace_row).astype(jnp.int32)
    fem_state = fem_field
    density = bem_density
    for sweep in range(ITERS):
        rounded = lax.optimization_barrier(density.astype(jnp.bfloat16))
        flat_fem = by_device(fem_state)
        traced = jnp.zeros((PANELS * PANEL, E), jnp.float32).at[node_index].add(flat_fem[cell_index])
        applied = near_field(rounded, near_blocks, near_pairs) + far_field(rounded, low_left, low_right, centers, near_pairs) + traced.T
        coupled_flat = jnp.zeros((N_FEM * N_BEM * CX * CY * CZ, E), jnp.float32).at[cell_index].add(density.T[node_index])
        coupled = from_device(coupled_flat)
        fem_next = fem_state + (fem_source - stiffness(fem_state, reaction) - coupled) / (6.0 + reaction)[..., None]
        density = density + (bem_source - applied) / bem_diagonal[None, :]
        fem_state = fem_next
    return fem_state, density
```

```python
import jax
import jax.numpy as jnp
from jax import lax
from jax.experimental import pallas as pl
from jax.experimental.pallas import tpu as pltpu
from jax.sharding import PartitionSpec as P

CAP = 32
ITERS = 3


HIGHEST = lax.Precision.HIGHEST


def faces(x, axis, dim):
    size, length = (lax.axis_size(axis), x.shape[dim])
    up = [(i, (i + 1) % size) for i in range(size - 1)]
    down = [(j, i) for i, j in up]
    last = lax.slice_in_dim(x, length - 1, length, axis=dim).astype(jnp.bfloat16)
    initial = lax.slice_in_dim(x, 0, 1, axis=dim).astype(jnp.bfloat16)
    return lax.ppermute(last, axis, up), lax.ppermute(initial, axis, down)


def neighbour_sum(state, before_x, after_x, before_y, after_y):
    wide_x = jnp.concatenate(
        [before_x.astype(jnp.float32), state, after_x.astype(jnp.float32)], axis=0
    )
    wide_y = jnp.concatenate(
        [before_y.astype(jnp.float32), state, after_y.astype(jnp.float32)], axis=1
    )
    wide_z = jnp.pad(state, ((0, 0), (0, 0), (1, 1), (0, 0)))
    beside = wide_x[2:] + wide_x[:-2] + wide_y[:, 2:] + wide_y[:, :-2]
    return beside + wide_z[:, :, 2:] + wide_z[:, :, :-2]


def near_kernel(pairs_ref, x_ref, blocks_ref, init_ref, out_ref, acc_ref):
    p, k = pl.program_id(0), pl.program_id(1)

    @pl.when(k == 0)
    def _():
        acc_ref[...] = init_ref[...]

    acc_ref[...] += jnp.dot(
        x_ref[pairs_ref[p, k]], blocks_ref[0, 0], preferred_element_type=jnp.float32
    )

    @pl.when(k == pl.num_programs(1) - 1)
    def _():
        out_ref[...] = acc_ref[...].astype(out_ref.dtype)


def near_apply(pairs, x, blocks, init):
    panels, group, rows, cols = blocks.shape
    exc = x.shape[1]
    return pl.pallas_call(
        near_kernel,
        out_shape=jax.ShapeDtypeStruct((exc, panels * cols), jnp.bfloat16),
        grid_spec=pltpu.PrefetchScalarGridSpec(
            num_scalar_prefetch=1,
            grid=(panels, group),
            in_specs=[
                pl.BlockSpec(x.shape, lambda p, k, pairs: (0, 0, 0)),
                pl.BlockSpec((1, 1, rows, cols), lambda p, k, pairs: (p, k, 0, 0)),
                pl.BlockSpec((exc, cols), lambda p, k, pairs: (0, p)),
            ],
            out_specs=pl.BlockSpec((exc, cols), lambda p, k, pairs: (0, p)),
            scratch_shapes=[pltpu.VMEM((exc, cols), jnp.float32)],
        ),
        cost_estimate=pl.CostEstimate(
            flops=2 * exc * blocks.size, bytes_accessed=2 * blocks.size, transcendentals=0
        ),
        compiler_params=pltpu.CompilerParams(
            dimension_semantics=("arbitrary", "arbitrary"), vmem_limit_bytes=24 << 20
        ),
        name="near",
    )(pairs, x, blocks, init)


def pick_kernel(node_ref, x_ref, out_ref):
    panels, exc, rows = x_ref.shape
    slots = node_ref.shape[0]
    node = node_ref[...]
    lanes = lax.broadcasted_iota(jnp.int32, (slots, rows), 1)

    def step(q, acc):
        hot = jnp.where(lanes + q * rows == node, 1.0, 0.0).astype(jnp.bfloat16)
        return acc + lax.dot_general(
            hot, x_ref[q], (((1,), (1,)), ((), ())), preferred_element_type=jnp.float32
        )

    acc = lax.fori_loop(0, panels, step, jnp.zeros((slots, exc), jnp.float32))
    out_ref[...] = acc.astype(out_ref.dtype)


def pick_nodes(node, x):
    slots = node.shape[0]
    return pl.pallas_call(
        pick_kernel,
        out_shape=jax.ShapeDtypeStruct((slots, x.shape[1]), jnp.bfloat16),
        cost_estimate=pl.CostEstimate(
            flops=2 * slots * x.size, bytes_accessed=2 * x.size, transcendentals=0
        ),
        compiler_params=pltpu.CompilerParams(vmem_limit_bytes=24 << 20),
        name="pick",
    )(node, x)


def shards(
    fem_field,
    fem_source,
    reaction,
    bem_density,
    bem_source,
    bem_diagonal,
    near_blocks,
    near_pairs,
    low_left,
    low_right,
    centers,
    trace_cell,
    trace_bank,
    trace_row,
):
    fem_count = lax.axis_size("fem")
    bem_count = lax.axis_size("bem")
    fem_rank = lax.axis_index("fem")
    bem_rank = lax.axis_index("bem")
    excitations, local_rows = bem_density.shape
    share_cols = excitations // fem_count
    local_panels = near_blocks.shape[0]
    group_size = near_blocks.shape[1]
    panel_rows = near_blocks.shape[2]
    panel_total = low_right.shape[0]
    cell_total = reaction.size
    slot_total = trace_cell.shape[0]
    first_col = fem_rank * share_cols
    slot_bank = trace_bank[:, 0]
    positions = jnp.arange(slot_total, dtype=jnp.int32)
    earlier = (slot_bank[:, None] == slot_bank[None, :]) & (positions[None, :] < positions[:, None])
    slot_place = jnp.sum(earlier.astype(jnp.int32), axis=1)
    destination = slot_bank * CAP + slot_place
    places = jnp.arange(bem_count * CAP, dtype=jnp.int32)[:, None] == destination[None, :]
    send_rows = jnp.sum(jnp.where(places, trace_row[None, :] + 1, 0), axis=1) - 1
    send_cell = jnp.sum(jnp.where(places, trace_cell[None, :] + 1, 0), axis=1) - 1
    recv_rows = lax.all_to_all(
        send_rows.reshape(bem_count, CAP), "bem", split_axis=0, concat_axis=0, tiled=True
    )
    cell_ids = jnp.arange(cell_total, dtype=jnp.int32)
    send_hot = (send_cell[:, None] == cell_ids[None, :]).astype(jnp.bfloat16)
    cell_hot = (cell_ids[:, None] == trace_cell[None, :]).astype(jnp.bfloat16)
    row_ids = jnp.arange(local_rows, dtype=jnp.int32)
    recv_hot = (recv_rows.reshape(-1)[:, None] == row_ids[None, :]).astype(jnp.bfloat16)
    node = (slot_bank * local_rows + trace_row)[:, None]
    own_first = bem_rank * local_panels
    own_centers = lax.dynamic_slice_in_dim(centers, own_first, local_panels, 0)
    offsets = own_centers[:, None, :] - centers[None, :, :]
    kernel_rows = 1.0 / (1.0 + jnp.sum(offsets * offsets, axis=-1))
    panel_ids = jnp.arange(panel_total, dtype=jnp.int32)
    own_ids = own_first + jnp.arange(local_panels, dtype=jnp.int32)
    listed = jnp.any(near_pairs[:, :, None] == panel_ids[None, None, :], axis=1)
    listed = listed | (own_ids[:, None] == panel_ids[None, :])
    kernel_rows = jnp.where(listed, 0.0, kernel_rows)
    left_wide = low_left.astype(jnp.float32)
    pair_group = lax.dynamic_slice_in_dim(near_pairs, fem_rank * group_size, group_size, 1)
    density = lax.dynamic_slice_in_dim(bem_density, first_col, share_cols, 0)
    source_part = lax.dynamic_slice_in_dim(bem_source, first_col, share_cols, 0)
    diag_row = bem_diagonal[None, :]
    fem_state = fem_field
    for sweep in range(ITERS):
        whole = bem_density if sweep == 0 else density
        narrow = whole.astype(jnp.bfloat16).reshape(-1, local_panels, panel_rows)
        narrow = jnp.transpose(narrow, (1, 0, 2))
        if sweep > 0:
            narrow = lax.all_gather(narrow, "fem", axis=1, tiled=True)
        x = lax.all_gather(narrow, "bem", axis=0, tiled=True)
        before_x, after_x = faces(fem_state, "fem", 0)
        before_y, after_y = faces(fem_state, "bem", 1)
        outgoing = jnp.dot(
            send_hot,
            fem_state.astype(jnp.bfloat16).reshape(cell_total, excitations),
            preferred_element_type=jnp.float32,
        ).astype(jnp.bfloat16)
        incoming = lax.all_to_all(
            outgoing.reshape(bem_count, CAP, excitations),
            "bem",
            split_axis=0,
            concat_axis=0,
            tiled=True,
        )
        traced = lax.dot_general(
            incoming.reshape(-1, excitations),
            recv_hot,
            (((0,), (0,)), ((), ())),
            preferred_element_type=jnp.float32,
        )
        partial_sum = near_apply(pair_group, x, near_blocks, traced)
        parts = lax.all_to_all(
            partial_sum.reshape(fem_count, share_cols, local_rows),
            "fem",
            split_axis=0,
            concat_axis=0,
            tiled=True,
        )
        own_cols = lax.dynamic_slice_in_dim(x, first_col, share_cols, 1)
        reduced = jnp.einsum(
            "qen,qrn->qer", own_cols, low_right, preferred_element_type=jnp.float32
        ).astype(jnp.bfloat16)
        reduced = lax.optimization_barrier(reduced).astype(jnp.float32)
        weights = jnp.einsum("pq,qer->per", kernel_rows, reduced, precision=HIGHEST)
        distant = jnp.einsum("per,prn->epn", weights, left_wide, precision=HIGHEST).reshape(
            share_cols, local_rows
        )
        values = pick_nodes(node, x)
        coupled = jnp.dot(cell_hot, values, preferred_element_type=jnp.float32).reshape(
            fem_state.shape
        )
        scale = (6.0 + reaction)[..., None]
        beside = neighbour_sum(fem_state, before_x, after_x, before_y, after_y)
        fem_next = fem_state + (fem_source - (scale * fem_state - beside) - coupled) / scale
        applied = distant + jnp.sum(parts.astype(jnp.float32), axis=0)
        density = density + (source_part - applied) / diag_row
        fem_state = fem_next
    return (fem_state, density)


def solution(mesh):
    return jax.shard_map(
        shards,
        mesh=mesh,
        in_specs=(
            P("fem", "bem", None, None),
            P("fem", "bem", None, None),
            P("fem", "bem", None),
            P(None, "bem"),
            P(None, "bem"),
            P("bem"),
            P("bem", "fem", None, None),
            P("bem", None),
            P("bem", None, None),
            P(),
            P(),
            P(("fem", "bem")),
            P(("fem", "bem"), None),
            P(("fem", "bem")),
        ),
        out_specs=(P("fem", "bem", None, None), P("fem", "bem")),
        check_vma=False,
    )
```

```python
import functools

import jax
import jax.numpy as jnp
from jax import lax
from jax.experimental import pallas as pl
from jax.experimental.pallas import tpu as pltpu
from jax.sharding import PartitionSpec as P

CAP = 32
ITERS = 3


HIGHEST = lax.Precision.HIGHEST
MESH = pl.DeviceIdType.MESH


def exchange_kernel(plan, count, *refs):
    items = len(plan)
    sources, targets = refs[:items], refs[items : 2 * items]
    send_sem, recv_sem, own_sem = refs[2 * items :]
    sizes = {axis: lax.axis_size(axis) for axis in ("fem", "bem")}
    ranks = {axis: lax.axis_index(axis) for axis in ("fem", "bem")}

    def device(axis, step):
        place = dict(ranks)
        place[axis] = lax.rem(ranks[axis] + step, sizes[axis])
        return (place["fem"], place["bem"])

    def steps(kind, axis):
        return [kind % sizes[axis]] if isinstance(kind, int) else range(1, sizes[axis])

    peers = sorted({(axis, step) for kind, axis in plan for step in steps(kind, axis)})
    barrier = pltpu.get_barrier_semaphore()
    for axis, step in peers:
        pl.semaphore_signal(barrier, inc=1, device_id=device(axis, step), device_id_type=MESH)
    pl.semaphore_wait(barrier, len(peers))

    def own_place(kind, axis, source, target):
        rank = ranks[axis]
        if kind == "gather":
            rows = source.shape[1]
            return target.at[:, pl.ds(pl.multiple_of(rank * rows, rows), rows), :]
        return target.at[rank] if kind == "scatter" else target

    copies = []
    for (kind, axis), source, target in zip(plan, sources, targets):
        for step in steps(kind, axis):
            place = device(axis, step)
            there = place[0] if axis == "fem" else place[1]
            slot = len(copies)
            copy = pltpu.make_async_remote_copy(
                src_ref=source.at[there] if kind == "scatter" else source,
                dst_ref=own_place(kind, axis, source, target),
                send_sem=send_sem.at[slot],
                recv_sem=recv_sem.at[slot],
                device_id=place,
                device_id_type=MESH,
            )
            copy.start()
            copies.append(copy)
    for item, ((kind, axis), source, target) in enumerate(zip(plan, sources, targets)):
        if not isinstance(kind, int):
            copy = pltpu.make_async_copy(
                source.at[ranks[axis]] if kind == "scatter" else source,
                own_place(kind, axis, source, target),
                own_sem.at[item],
            )
            copy.start()
            copies.append(copy)
    for copy in copies:
        copy.wait()


def exchange(plan, arrays, name, collective_id):
    shapes, count = [], 0
    for (kind, axis), x in zip(plan, arrays):
        size = lax.axis_size(axis)
        count += 1 if isinstance(kind, int) else size - 1
        shape = (x.shape[0], x.shape[1] * size, x.shape[2]) if kind == "gather" else x.shape
        shapes.append(jax.ShapeDtypeStruct(shape, x.dtype))
    return pl.pallas_call(
        functools.partial(exchange_kernel, plan, count),
        out_shape=shapes,
        in_specs=[pl.BlockSpec(memory_space=pltpu.VMEM)] * len(arrays),
        out_specs=[pl.BlockSpec(memory_space=pltpu.VMEM)] * len(arrays),
        scratch_shapes=[
            pltpu.SemaphoreType.DMA((count,)),
            pltpu.SemaphoreType.DMA((count,)),
            pltpu.SemaphoreType.DMA((len(plan),)),
        ],
        cost_estimate=pl.CostEstimate(
            flops=1 << 29, bytes_accessed=sum(x.size for x in arrays) * 4, transcendentals=0
        ),
        compiler_params=pltpu.CompilerParams(
            collective_id=collective_id, has_side_effects=True, vmem_limit_bytes=8 << 20
        ),
        name=name,
    )(*arrays)


def end_faces(state):
    narrow = lambda x: x.astype(jnp.bfloat16)
    return [narrow(state[-1:]), narrow(state[:1]), narrow(state[:, -1:]), narrow(state[:, :1])]


FACE_PLAN = ((1, "fem"), (-1, "fem"), (1, "bem"), (-1, "bem"))


def neighbour_sum(state, before_x, after_x, before_y, after_y):
    wide_x = jnp.concatenate(
        [before_x.astype(jnp.float32), state, after_x.astype(jnp.float32)], axis=0
    )
    wide_y = jnp.concatenate(
        [before_y.astype(jnp.float32), state, after_y.astype(jnp.float32)], axis=1
    )
    wide_z = jnp.pad(state, ((0, 0), (0, 0), (1, 1), (0, 0)))
    beside = wide_x[2:] + wide_x[:-2] + wide_y[:, 2:] + wide_y[:, :-2]
    return beside + wide_z[:, :, 2:] + wide_z[:, :, :-2]


def near_kernel(pairs_ref, x_ref, blocks_ref, init_ref, out_ref, acc_ref):
    p, k = pl.program_id(0), pl.program_id(1)

    @pl.when(k == 0)
    def _():
        acc_ref[...] = init_ref[...]

    width = blocks_ref.shape[1]
    acc = acc_ref[...]
    for i in range(width):
        acc += jnp.dot(
            x_ref[pairs_ref[p, k * width + i]],
            blocks_ref[0, i],
            preferred_element_type=jnp.float32,
        )
    acc_ref[...] = acc

    @pl.when(k == pl.num_programs(1) - 1)
    def _():
        out_ref[...] = acc_ref[...].astype(out_ref.dtype)


def near_apply(pairs, x, blocks, init):
    panels, group, rows, cols = blocks.shape
    exc = x.shape[1]
    width = next(w for w in (4, 3, 2, 1) if group % w == 0)
    return pl.pallas_call(
        near_kernel,
        out_shape=jax.ShapeDtypeStruct((exc, panels * cols), jnp.bfloat16),
        grid_spec=pltpu.PrefetchScalarGridSpec(
            num_scalar_prefetch=1,
            grid=(panels, group // width),
            in_specs=[
                pl.BlockSpec(x.shape, lambda p, k, pairs: (0, 0, 0)),
                pl.BlockSpec((1, width, rows, cols), lambda p, k, pairs: (p, k, 0, 0)),
                pl.BlockSpec((exc, cols), lambda p, k, pairs: (0, p)),
            ],
            out_specs=pl.BlockSpec((exc, cols), lambda p, k, pairs: (0, p)),
            scratch_shapes=[pltpu.VMEM((exc, cols), jnp.float32)],
        ),
        cost_estimate=pl.CostEstimate(
            flops=2 * exc * blocks.size, bytes_accessed=2 * blocks.size, transcendentals=0
        ),
        compiler_params=pltpu.CompilerParams(
            dimension_semantics=("arbitrary", "arbitrary"), vmem_limit_bytes=52 << 20
        ),
        name="near",
    )(pairs, x, blocks, init)


def pick_kernel(node_ref, x_ref, out_ref):
    panels, exc, rows = x_ref.shape
    slots = node_ref.shape[1]
    node = node_ref[...]
    places = lax.broadcasted_iota(jnp.int32, (rows, slots), 0)

    def step(q, acc):
        hot = jnp.where(places == node - q * rows, 1.0, 0.0).astype(jnp.bfloat16)
        return acc + jnp.dot(x_ref[q], hot, preferred_element_type=jnp.float32)

    acc = lax.fori_loop(0, panels, step, jnp.zeros((exc, slots), jnp.float32), unroll=2)
    out_ref[...] = acc.astype(out_ref.dtype)


def pick_nodes(node, x):
    slots = node.shape[1]
    return pl.pallas_call(
        pick_kernel,
        out_shape=jax.ShapeDtypeStruct((x.shape[1], slots), jnp.bfloat16),
        cost_estimate=pl.CostEstimate(
            flops=2 * slots * x.size, bytes_accessed=2 * x.size, transcendentals=0
        ),
        compiler_params=pltpu.CompilerParams(vmem_limit_bytes=24 << 20),
        name="pick",
    )(node, x)


def shards(
    fem_field,
    fem_source,
    reaction,
    bem_density,
    bem_source,
    bem_diagonal,
    near_blocks,
    near_pairs,
    low_left,
    low_right,
    centers,
    trace_cell,
    trace_bank,
    trace_row,
):
    fem_count = lax.axis_size("fem")
    bem_count = lax.axis_size("bem")
    fem_rank = lax.axis_index("fem")
    bem_rank = lax.axis_index("bem")
    excitations, local_rows = bem_density.shape
    share_cols = excitations // fem_count
    local_panels = near_blocks.shape[0]
    group_size = near_blocks.shape[1]
    panel_rows = near_blocks.shape[2]
    panel_total = low_right.shape[0]
    cell_total = reaction.size
    slot_total = trace_cell.shape[0]
    first_col = fem_rank * share_cols
    slot_bank = trace_bank[:, 0]
    positions = jnp.arange(slot_total, dtype=jnp.int32)
    earlier = (slot_bank[:, None] == slot_bank[None, :]) & (positions[None, :] < positions[:, None])
    slot_place = jnp.sum(earlier.astype(jnp.int32), axis=1)
    destination = slot_bank * CAP + slot_place
    places = jnp.arange(bem_count * CAP, dtype=jnp.int32)[:, None] == destination[None, :]
    send_rows = jnp.sum(jnp.where(places, trace_row[None, :] + 1, 0), axis=1) - 1
    send_cell = jnp.sum(jnp.where(places, trace_cell[None, :] + 1, 0), axis=1) - 1
    rows_wide = jnp.full((bem_count, 8, 128), -1, jnp.int32)
    rows_wide = rows_wide.at[:, :, :CAP].set(send_rows.reshape(bem_count, 1, CAP))
    cell_ids = jnp.arange(cell_total, dtype=jnp.int32)
    send_hot = (send_cell[:, None] == cell_ids[None, :]).astype(jnp.bfloat16)
    cell_hot = (cell_ids[:, None] == trace_cell[None, :]).astype(jnp.bfloat16)
    row_ids = jnp.arange(local_rows, dtype=jnp.int32)
    node = (slot_bank * local_rows + trace_row)[None, :]
    own_first = bem_rank * local_panels
    own_centers = lax.dynamic_slice_in_dim(centers, own_first, local_panels, 0)
    offsets = own_centers[:, None, :] - centers[None, :, :]
    kernel_rows = 1.0 / (1.0 + jnp.sum(offsets * offsets, axis=-1))
    panel_ids = jnp.arange(panel_total, dtype=jnp.int32)
    own_ids = own_first + jnp.arange(local_panels, dtype=jnp.int32)
    listed = jnp.any(near_pairs[:, :, None] == panel_ids[None, None, :], axis=1)
    listed = listed | (own_ids[:, None] == panel_ids[None, :])
    kernel_rows = jnp.where(listed, 0.0, kernel_rows)
    left_wide = low_left.astype(jnp.float32)
    pair_group = lax.dynamic_slice_in_dim(near_pairs, fem_rank * group_size, group_size, 1)
    density = lax.dynamic_slice_in_dim(bem_density, first_col, share_cols, 0)
    source_part = lax.dynamic_slice_in_dim(bem_source, first_col, share_cols, 0)
    diag_row = bem_diagonal[None, :]
    fem_state = fem_field
    for sweep in range(ITERS):
        whole = bem_density if sweep == 0 else density
        narrow = whole.astype(jnp.bfloat16).reshape(-1, local_panels, panel_rows)
        narrow = jnp.transpose(narrow, (1, 0, 2))
        if sweep > 0:
            (narrow,) = exchange((("gather", "fem"),), [narrow], "share_gather", 1)
        x = lax.all_gather(narrow, "bem", axis=0, tiled=True)
        outgoing = jnp.dot(
            send_hot,
            fem_state.astype(jnp.bfloat16).reshape(cell_total, excitations),
            preferred_element_type=jnp.float32,
        ).astype(jnp.bfloat16)
        arrays = [*end_faces(fem_state), outgoing.reshape(bem_count, CAP, excitations)]
        plan = (*FACE_PLAN, ("scatter", "bem"))
        if sweep == 0:
            *layers, incoming, recv_rows = exchange(
                (*plan, ("scatter", "bem")), [*arrays, rows_wide], "first_exchange", 0
            )
            recv_rows = recv_rows[:, 0, :CAP].reshape(-1)
            recv_hot = (recv_rows[:, None] == row_ids[None, :]).astype(jnp.bfloat16)
        else:
            *layers, incoming = exchange(plan, arrays, "layer_exchange", 2)
        inside = (fem_rank > 0, fem_rank < fem_count - 1, bem_rank > 0, bem_rank < bem_count - 1)
        layers = [
            jnp.where(here, x, jnp.zeros_like(x)) for here, x in zip(inside, layers)
        ]
        traced = lax.dot_general(
            incoming.reshape(-1, excitations),
            recv_hot,
            (((0,), (0,)), ((), ())),
            preferred_element_type=jnp.float32,
        )
        partial_sum = near_apply(pair_group, x, near_blocks, traced)
        (parts,) = exchange(
            (("scatter", "fem"),),
            [partial_sum.reshape(fem_count, share_cols, local_rows)],
            "part_scatter",
            3,
        )
        own_cols = lax.dynamic_slice_in_dim(x, first_col, share_cols, 1)
        reduced = jnp.einsum(
            "qen,qrn->qer", own_cols, low_right, preferred_element_type=jnp.float32
        ).astype(jnp.bfloat16)
        reduced = lax.optimization_barrier(reduced).astype(jnp.float32)
        weights = jnp.einsum("pq,qer->per", kernel_rows, reduced, precision=HIGHEST)
        distant = jnp.einsum("per,prn->epn", weights, left_wide, precision=HIGHEST).reshape(
            share_cols, local_rows
        )
        values = pick_nodes(node, x)
        coupled = lax.dot_general(
            cell_hot, values, (((1,), (1,)), ((), ())), preferred_element_type=jnp.float32
        ).reshape(fem_state.shape)
        scale = (6.0 + reaction)[..., None]
        beside = neighbour_sum(fem_state, *layers)
        fem_next = fem_state + (fem_source - (scale * fem_state - beside) - coupled) / scale
        applied = distant + jnp.sum(parts.astype(jnp.float32), axis=0)
        density = density + (source_part - applied) / diag_row
        fem_state = fem_next
    return (fem_state, density)


def solution(mesh):
    return jax.shard_map(
        shards,
        mesh=mesh,
        in_specs=(
            P("fem", "bem", None, None),
            P("fem", "bem", None, None),
            P("fem", "bem", None),
            P(None, "bem"),
            P(None, "bem"),
            P("bem"),
            P("bem", "fem", None, None),
            P("bem", None),
            P("bem", None, None),
            P(),
            P(),
            P(("fem", "bem")),
            P(("fem", "bem"), None),
            P(("fem", "bem")),
        ),
        out_specs=(P("fem", "bem", None, None), P("fem", "bem")),
        check_vma=False,
    )
```
